32 devices in a mesh: expert: 4 (over y, x), shard: 8 (over z, core).
Axes of the slice: x: 2, y: 2, z: 4, core: 2. Of those that a mesh axis runs over, the one named last changes fastest.
Arguments:
- tokens: bfloat16 [256, 6144], P(('expert', 'shard')), may hold values from -6 to 6
- norm_gain: float32 [6144], replicated, may hold values from 0.5 to 1.5
- routes: int32 [256, 2], P(('expert', 'shard')), may hold values from 0 to 3, all different within a row; in each aligned block of 8 rows (0 to 7, 8 to 15, ...) at most 4 rows name the same one
- gate_weights: float32 [256, 2], P(('expert', 'shard')), may hold values from 0.2 to 1
- capacity: int32 [4], replicated, may hold values from 2 to 4
- w_gate: bfloat16 [4, 6144, 8192], P('expert', None, 'shard'), may hold values from -0.078125 to 0.078125
- w_up: bfloat16 [4, 6144, 8192], P('expert', None, 'shard'), may hold values from -0.078125 to 0.078125
- w_down: bfloat16 [4, 8192, 6144], P('expert', 'shard'), may hold values from -0.0625 to 0.0625
Outputs:
- mixed_out: bfloat16 [256, 6144], P(('expert', 'shard'))
The draws below stay inside these ranges and needn't reach their ends.
Inputs may be any that keep to these rules, and one draw needn't show every extreme that they name: `routes`: each row names 2 different experts; among the rows of one device no expert is named by more than 4 rows.
All inputs are finite; a program needn't handle non-finite values.
Results may differ from the reference program's by a relative error of at most 0.019.
Values may be sent and summed in bfloat16 or wider, within the bound.
A program may use at most 128 MiB of HBM per device.

```python
import math
import jax
import jax.numpy as jnp
import numpy as np
from jax import lax

D = 6144
FF = 8192
TOPK = 2
TOK_DEV = 8
EXPERTS = 4
MOST = 4
TOKENS = 256
N_SHARD = 8


def draw_capacity(key, part):
    drawn_caps = jax.random.randint(key, (EXPERTS,), MOST // 2, MOST + 1, dtype=jnp.int32)
    chosen = jax.random.randint(jax.random.fold_in(key, 7), (), 0, EXPERTS, dtype=jnp.int32)
    return jnp.where(jnp.arange(EXPERTS, dtype=jnp.int32) == chosen, MOST, drawn_caps).astype(jnp.int32)


def levels(rng, extent, shards, low, high):
    level, own = 1.0, jax.random.fold_in(rng, 6)
    for dim, blocks in shards:
        draws = jnp.exp(jax.random.uniform(jax.random.fold_in(own, dim), (blocks,), jnp.float32, low / len(shards), high / len(shards)))
        level = level * jnp.repeat(draws, extent[dim] // blocks).reshape([-1 if axis == dim else 1 for axis in range(len(extent))])
    return level


def assign_block(own_key, own, number, rows, amount, top, bound, skew):
    order = jax.random.permutation(own_key, amount)
    packed, usual = portions_of(amount, rows * top, bound, skew, True), portions_of(amount, rows * top, bound, skew, False)
    places = jnp.arange(amount)

    def named(tallies, offset_by):
        used = int((tallies > 0).sum())
        fixed = max(1, used // 4)
        passed = fixed + (places - fixed + offset_by * (used - fixed)) % max(1, amount - fixed)
        return jnp.zeros((amount,), jnp.int32).at[order[jnp.where(places < fixed, places, passed)]].set(jnp.asarray(tallies, jnp.int32))

    tallies = jnp.where(number % 4 == 0, named(packed, number // 4), named(usual, number - number // 4 - 1))
    mixed = jax.random.permutation(jax.random.fold_in(own, 3), amount)
    giver, sink = mixed[0:amount // 2 * 2:2], mixed[1:amount // 2 * 2:2]
    margin = jnp.minimum(tallies[giver] - 1, bound - tallies[sink]) // 2
    margin = jnp.where((giver == order[0]) | (sink == order[0]) | (tallies[sink] == 0), 0, jnp.maximum(margin, 0))
    passed = jax.random.randint(jax.random.fold_in(own, 4), (amount // 2,), 0, 1 << 20) % (margin + 1)
    tallies = tallies.at[giver].add(-passed).at[sink].add(passed)
    members = jnp.searchsorted(jnp.cumsum(tallies), jnp.arange(rows * top), side="right").astype(jnp.int32)
    listing = members.reshape(top, rows).T
    listing = listing[jax.random.permutation(jax.random.fold_in(own, 1), rows)]
    offset_by = jax.random.randint(jax.random.fold_in(own, 2), (rows, 1), 0, top)
    return jnp.take_along_axis(listing, (jnp.arange(top)[None, :] + offset_by) % top, axis=1)


def portions_of(amount, total, bound, lean, full):
    weights = [(1 << 20) // math.isqrt(standing ** lean) + 1 for standing in range(1, amount + 1)]
    largest = bound if full else min(bound, max(-(-total // amount), total * weights[0] // sum(weights)))
    least = 1 if total - largest >= amount - 1 else 0
    holding, surplus = [largest] + [least] * (amount - 1), total - largest - least * (amount - 1)
    while surplus > 0:
        free = [i for i in range(1, amount) if holding[i] < largest] or [i for i in range(1, amount) if holding[i] < bound]
        mass, budget = sum([weights[i] for i in free]), surplus
        for i in free:
            extra = min(bound - holding[i], max(1, budget * weights[i] // mass), surplus)
            holding[i] = holding[i] + extra
            surplus = surplus - extra
    return np.array(holding)


def centred(key, dims, scale, limit, cuts=(), held_as=jnp.bfloat16):
    gain = levels(key, dims, cuts, -0.22, 0.18) if cuts else 1.0
    result = jax.random.normal(key, dims, jnp.float32) * scale * gain
    return jnp.minimum(jnp.maximum(result, -limit), limit).astype(held_as)


def setup_inputs(seed: int = 0) -> dict:
    keys = jax.random.split(jax.random.key(seed), 9)
    tokens = centred(keys[0], (TOKENS, D), 1.0, 6.0, ((0, 32),))
    norm_gain = jnp.clip(1.0 + 0.1 * jax.random.normal(keys[1], (D,), jnp.float32), 0.5, 1.5)
    routes_keys = jax.random.split(jax.random.fold_in(keys[2], 1), TOKENS // TOK_DEV)
    routes_turns = jax.random.permutation(jax.random.fold_in(keys[2], 3), TOKENS // TOK_DEV)
    routes = jax.vmap(lambda own, number: assign_block(jax.random.fold_in(keys[2], 2), own, number, TOK_DEV, EXPERTS, TOPK, MOST, 2))(routes_keys, routes_turns).reshape((TOKENS, TOPK))
    gate_weights = jnp.clip(jnp.exp(math.log(1.0) - 1.609438 * jax.random.uniform(keys[3], (TOKENS, TOPK), jnp.float32) ** levels(keys[3], (TOKENS, TOPK), ((0, 32),), -0.2, 0.2)), 0.2, 1.0)
    capacity = draw_capacity(jax.random.fold_in(keys[8], 71), 0)
    w_gate = centred(keys[5], (EXPERTS, D, FF), D ** -0.5, 0.078125, ((0, 4), (2, 8)))
    w_up = centred(keys[6], (EXPERTS, D, FF), D ** -0.5, 0.078125, ((0, 4), (2, 8)))
    w_down = centred(keys[7], (EXPERTS, FF, D), FF ** -0.5, 0.0625, ((0, 4), (1, 8)))
    return {"tokens": tokens, "norm_gain": norm_gain, "routes": routes, "gate_weights": gate_weights, "capacity": capacity, "w_gate": w_gate, "w_up": w_up, "w_down": w_down}


def rms_norm(tokens, norm_gain):
    widened = tokens.astype(jnp.float32)
    mean_square = lax.optimization_barrier(jnp.mean(widened * widened, axis=-1, keepdims=True))
    return (widened * lax.rsqrt(mean_square + 1e-05) * norm_gain).astype(jnp.bfloat16)

def slot_ranks(blocked):
    equal_ids = blocked[:, :, None, :, None] == blocked[:, None, :, None, :]
    shared = jnp.any(equal_ids, axis=4).astype(jnp.int32)
    per_block = blocked.shape[1]
    positions = jnp.arange(per_block, dtype=jnp.int32)
    earlier = (positions[None, :] < positions[:, None]).astype(jnp.int32)
    return lax.optimization_barrier(jnp.sum(shared * earlier[None, :, :, None], axis=2)).astype(jnp.int32)

def expert_apply(buffer, gate_proj, up_proj, down_proj):
    gate_val = jnp.dot(buffer, gate_proj, preferred_element_type=jnp.float32)
    up_val = jnp.dot(buffer, up_proj, preferred_element_type=jnp.float32)
    hidden = (jax.nn.silu(gate_val) * up_val).astype(jnp.bfloat16)
    hidden_width = FF // N_SHARD

    def add_shard(running, shard_idx):
        start_col = (shard_idx * hidden_width).astype(jnp.int32)
        hidden_part = lax.dynamic_slice_in_dim(hidden, start_col, hidden_width, 1)
        down_part = lax.dynamic_slice_in_dim(down_proj, start_col, hidden_width, 0)
        rounded = jnp.dot(hidden_part, down_part, preferred_element_type=jnp.float32).astype(jnp.bfloat16)
        rounded = lax.optimization_barrier(rounded)
        return (running + rounded.astype(jnp.float32), None)
    initial = jnp.zeros((buffer.shape[0], down_proj.shape[1]), jnp.float32)
    running, _ = lax.scan(add_shard, initial, jnp.arange(N_SHARD, dtype=jnp.int32))
    return running.astype(jnp.bfloat16)

def reference(tokens, norm_gain, routes, gate_weights, capacity, w_gate, w_up, w_down):
    normed = rms_norm(tokens, norm_gain)
    nblocks = TOKENS // TOK_DEV
    slot_rank = slot_ranks(routes.reshape(nblocks, TOK_DEV, TOPK)).reshape(TOKENS, TOPK)
    kept_mask = slot_rank < capacity[routes]
    block_ids = (jnp.arange(TOKENS, dtype=jnp.int32) // TOK_DEV)[:, None]
    slot_index = (block_ids * MOST + slot_rank).astype(jnp.int32)
    dump_row = nblocks * MOST
    mixed_out = jnp.zeros((TOKENS, D), jnp.float32)
    for expert_idx in range(EXPERTS):
        routed_mask = kept_mask & (routes == expert_idx)
        dest_rows = jnp.where(routed_mask, slot_index, dump_row).astype(jnp.int32)
        buffer = jnp.zeros((dump_row + 1, D), jnp.bfloat16)
        for slot_k in range(TOPK):
            buffer = buffer.at[dest_rows[:, slot_k]].set(normed)
        expert_out = expert_apply(buffer, w_gate[expert_idx], w_up[expert_idx], w_down[expert_idx])
        for slot_k in range(TOPK):
            taken = expert_out[dest_rows[:, slot_k]].astype(jnp.float32)
            weighted = gate_weights[:, slot_k:slot_k + 1] * taken
            mixed_out = mixed_out + jnp.where(routed_mask[:, slot_k:slot_k + 1], weighted, jnp.float32(0.0))
    return mixed_out.astype(jnp.bfloat16)
```

```python
import functools

import jax
import jax.numpy as jnp
from jax import lax
from jax.experimental import pallas as pl
from jax.experimental.pallas import tpu as pltpu
from jax.sharding import PartitionSpec as P

CHUNKS = 4
EPS = 1e-05
MESH = pl.DeviceIdType.MESH
CORES = 2


def column_tile(width, most):
    tile = most
    while width % tile:
        tile //= 2
    return tile


def kernel(
    n_expert, n_line, depth,
    tokens, gain, routes, gates, capacity, gate_hbm, up_hbm, down_hbm, out,
    gate_w, up_w, down_w, meta, normed, picked, rows, acc_gate, acc_up, hidden, partner, summed, returned, mixed, final,
    w_sem, meta_send, meta_recv, line_send, line_recv, plane_send, plane_recv, relay_send, relay_recv,
    pair_send, pair_recv, back_send, back_recv, home_send, home_recv,
):
    expert = lax.axis_index("expert")
    shard = lax.axis_index("shard")
    place, core = shard // CORES, lax.rem(shard, CORES)
    other = 1 - core
    tok, width = tokens.shape
    cols = width // CHUNKS
    slots = n_line * depth
    used = n_expert * slots
    lanes = meta.shape[2]
    hid = gate_w.shape[1]
    total_rows = CORES * used

    def line_at(step):
        return lax.rem(place + step + n_line, n_line)

    def expert_at(step):
        return lax.rem(expert + step + n_expert, n_expert)

    def line_device(step):
        return {"expert": expert, "shard": line_at(step) * CORES + core}

    def plane_device(step):
        return {"expert": expert_at(step), "shard": shard}

    partner_device = {"expert": expert, "shard": place * CORES + other}
    peers = [line_device(d) for d in range(1, n_line)] + [plane_device(d) for d in range(1, n_expert)] + [partner_device]

    barrier = pltpu.get_barrier_semaphore()
    for peer in peers:
        pl.semaphore_signal(barrier, inc=1, device_id=peer, device_id_type=MESH)

    def weight_copy(kind, step):
        span = pl.ds(step * cols, cols)
        if kind == 0:
            return pltpu.make_async_copy(gate_hbm.at[0, span, :], gate_w.at[span, :], w_sem.at[0, step])
        if kind == 1:
            return pltpu.make_async_copy(up_hbm.at[0, span, :], up_w.at[span, :], w_sem.at[1, step])
        return pltpu.make_async_copy(down_hbm.at[0, :, span], down_w.at[:, span], w_sem.at[2, step])

    for step in range(CHUNKS):
        weight_copy(0, step).start()
        weight_copy(1, step).start()
    for step in range(CHUNKS):
        weight_copy(2, step).start()

    lane = lax.broadcasted_iota(jnp.int32, (tok, lanes), 1)
    row = lax.broadcasted_iota(jnp.int32, (tok, lanes), 0)
    lane_expert = lane // slots
    lane_slot = lax.rem(lane, depth)
    first = routes[:, 0:1] == lane_expert
    named = first.astype(jnp.float32)
    weight = jnp.where(first, gates[:, 0:1], 0.0)
    for k in range(1, routes.shape[1]):
        this = routes[:, k : k + 1] == lane_expert
        named = jnp.maximum(named, this.astype(jnp.float32))
        weight = jnp.where(this, gates[:, k : k + 1], weight)
    rank = jnp.zeros((tok, lanes), jnp.float32)
    for t in range(tok - 1):
        rank = rank + jnp.where(row > t, named[t : t + 1, :], 0.0)
    limit = jnp.zeros((tok, lanes), jnp.int32)
    for e in range(n_expert):
        limit = jnp.where(lane_expert == e, capacity[e], limit)
    rank = rank.astype(jnp.int32)
    keep = (named > 0.0) & (rank == lane_slot) & (rank < limit)
    meta[place] = jnp.where(keep, weight, 0.0)

    wide = tokens[...].astype(jnp.float32)
    scale = lax.rsqrt(jnp.mean(wide * wide, axis=-1, keepdims=True) + EPS)
    values = (wide * scale * gain[...]).astype(jnp.bfloat16)
    for step in range(CHUNKS):
        normed[step, place] = values[:, step * cols : (step + 1) * cols]

    pl.semaphore_wait(barrier, len(peers))
    sent = []

    def remote(src, dst, send, recv, device):
        return pltpu.make_async_remote_copy(
            src_ref=src, dst_ref=dst, send_sem=send, recv_sem=recv, device_id=device, device_id_type=MESH
        )

    def send(*args):
        copy = remote(*args)
        copy.start()
        return copy

    for d in range(1, n_line):
        sent.append(send(meta.at[place], meta.at[place], meta_send.at[d - 1], meta_recv.at[d - 1], line_device(d)))
    for step in range(CHUNKS):
        for d in range(1, n_line):
            block = normed.at[step, place]
            sent.append(send(block, block, line_send.at[step, d - 1], line_recv.at[step, d - 1], line_device(d)))
    for d in range(1, n_line):
        block = meta.at[line_at(-d)]
        remote(block, block, meta_send.at[d - 1], meta_recv.at[d - 1], line_device(-d)).wait_recv()

    tall = n_line * tok
    all_meta = meta[...].reshape(tall, lanes)
    lane = lax.broadcasted_iota(jnp.int32, (tall, lanes), 1)
    row = lax.broadcasted_iota(jnp.int32, (tall, lanes), 0)
    combine = jnp.where(lax.rem(lane // depth, n_line) == row // tok, all_meta, 0.0)
    picker = (combine != 0.0).astype(jnp.float32).T[:used].astype(jnp.bfloat16)
    combine = combine.astype(jnp.bfloat16)[:, :used]

    tile = column_tile(cols, 512)
    relays = []

    def pick(step):
        for d in range(1, n_line):
            block = normed.at[step, line_at(-d)]
            remote(block, block, line_send.at[step, d - 1], line_recv.at[step, d - 1], line_device(-d)).wait_recv()

        def body(i, _):
            span = pl.ds(pl.multiple_of(i * tile, tile), tile)
            gathered = normed[step, :, :, span].astype(jnp.float32).reshape(tall, tile).astype(jnp.bfloat16)
            chosen = jnp.dot(picker, gathered, preferred_element_type=jnp.float32)
            picked[step, :, :, span] = chosen.astype(jnp.bfloat16).reshape(n_expert, slots, tile)
            return 0

        lax.fori_loop(0, cols // tile, body, 0)
        for d in range(1, n_expert):
            sent.append(
                send(
                    picked.at[step, expert_at(d)], rows.at[step, core, expert],
                    plane_send.at[step, d - 1], plane_recv.at[step, d - 1], plane_device(d),
                )
            )
        rows[step, core, expert] = picked[step, expert]
        block = rows.at[step, core, expert]
        relays.append(send(picked.at[step, expert], block, relay_send.at[step, 0], relay_recv.at[step, 0], partner_device))

    def relay(step):
        for d in range(1, n_expert):
            block = rows.at[step, core, expert_at(-d)]
            remote(block, block, plane_send.at[step, d - 1], plane_recv.at[step, d - 1], plane_device(-d)).wait_recv()
            relays.append(send(block, block, relay_send.at[step, d], relay_recv.at[step, d], partner_device))

    hid_tile = column_tile(hid, 256)

    def project(step):
        for d in range(n_expert):
            block = rows.at[step, other, expert_at(-d)]
            remote(block, block, relay_send.at[step, d], relay_recv.at[step, d], partner_device).wait_recv()
        weight_copy(0, step).wait()
        weight_copy(1, step).wait()

        def body(i, _):
            span = pl.ds(pl.multiple_of(i * hid_tile, hid_tile), hid_tile)
            x = rows[step].reshape(total_rows, cols)
            depth_span = pl.ds(step * cols, cols)
            g = jnp.dot(x, gate_w[depth_span, span], preferred_element_type=jnp.float32)
            u = jnp.dot(x, up_w[depth_span, span], preferred_element_type=jnp.float32)
            if step > 0:
                g = g + acc_gate[:, span]
                u = u + acc_up[:, span]
            if step < CHUNKS - 1:
                acc_gate[:, span] = g
                acc_up[:, span] = u
            else:
                hidden[:, span] = (g / (1.0 + jnp.exp(-g)) * u).astype(jnp.bfloat16)
            return 0

        lax.fori_loop(0, hid // hid_tile, body, 0)

    for i in range(CHUNKS + 2):
        if i < CHUNKS:
            pick(i)
        if 0 <= i - 1 < CHUNKS:
            relay(i - 1)
        if 0 <= i - 2 < CHUNKS:
            project(i - 2)
    for copy in relays:
        copy.wait_send()

    def down(step):
        weight_copy(2, step).wait()

        def body(i, _):
            span = pl.ds(pl.multiple_of(i * tile, tile), tile)
            w_span = pl.ds(pl.multiple_of(step * cols + i * tile, tile), tile)
            y = jnp.dot(hidden[...], down_w[:, w_span], preferred_element_type=jnp.float32)
            rows[step, :, :, :, span] = y.astype(jnp.bfloat16).reshape(CORES, n_expert, slots, tile)
            return 0

        lax.fori_loop(0, cols // tile, body, 0)
        sent.append(send(rows.at[step, other], partner.at[step], pair_send.at[step], pair_recv.at[step], partner_device))

    def pair(step):
        remote(rows.at[step, core], partner.at[step], pair_send.at[step], pair_recv.at[step], partner_device).wait_recv()
        for d in range(n_expert):
            e = expert_at(d)
            both = rows[step, core, e].astype(jnp.float32) + partner[step, e].astype(jnp.float32)
            if d == 0:
                returned[step, e] = both.astype(jnp.bfloat16)
            else:
                summed[step, e] = both.astype(jnp.bfloat16)
                sent.append(
                    send(
                        summed.at[step, e], returned.at[step, expert],
                        back_send.at[step, d - 1], back_recv.at[step, d - 1], plane_device(d),
                    )
                )

    def mix(step):
        for d in range(1, n_expert):
            block = returned.at[step, expert_at(-d)]
            remote(block, block, back_send.at[step, d - 1], back_recv.at[step, d - 1], plane_device(-d)).wait_recv()

        def body(i, _):
            span = pl.ds(pl.multiple_of(i * tile, tile), tile)
            r = returned[step, :, :, span].reshape(used, tile)
            o = jnp.dot(combine, r, preferred_element_type=jnp.float32)
            mixed[step, :, :, span] = o.reshape(n_line, tok, tile).astype(jnp.bfloat16)
            return 0

        lax.fori_loop(0, cols // tile, body, 0)
        for d in range(1, n_line):
            sent.append(
                send(
                    mixed.at[step, line_at(d)], final.at[step, place],
                    home_send.at[step, d - 1], home_recv.at[step, d - 1], line_device(d),
                )
            )

    def finish(step):
        total = mixed[step, place].astype(jnp.float32)
        for d in range(1, n_line):
            block = final.at[step, line_at(-d)]
            remote(block, block, home_send.at[step, d - 1], home_recv.at[step, d - 1], line_device(-d)).wait_recv()
        for d in range(1, n_line):
            total = total + final[step, line_at(-d)].astype(jnp.float32)
        out[:, step * cols : (step + 1) * cols] = total.astype(jnp.bfloat16)

    for i in range(CHUNKS + 1):
        if i < CHUNKS:
            down(i)
        if 0 <= i - 1 < CHUNKS:
            pair(i - 1)
    for i in range(CHUNKS):
        mix(i)
    for i in range(CHUNKS):
        finish(i)
    for copy in sent:
        copy.wait_send()


def solution(mesh):
    n_expert = mesh.shape["expert"]
    n_line = mesh.shape["shard"] // CORES

    def on_device(tokens, norm_gain, routes, gate_weights, capacity, w_gate, w_up, w_down):
        tok, width = tokens.shape
        hid = w_gate.shape[2]
        depth = max(tok // 2, tok * routes.shape[1] // n_expert)
        cols = width // CHUNKS
        slots = n_line * depth
        used = n_expert * slots
        lanes = -(-used // 128) * 128
        dma = pltpu.SemaphoreType.DMA
        bf16 = jnp.bfloat16
        vmem = pl.BlockSpec(memory_space=pltpu.VMEM)
        hbm = pl.BlockSpec(memory_space=pl.ANY)
        line, plane = (CHUNKS, n_line - 1), (CHUNKS, n_expert - 1)
        return pl.pallas_call(
            functools.partial(kernel, n_expert, n_line, depth),
            out_shape=jax.ShapeDtypeStruct((tok, width), bf16),
            in_specs=[vmem, vmem, vmem, vmem, pl.BlockSpec(memory_space=pltpu.SMEM), hbm, hbm, hbm],
            out_specs=vmem,
            scratch_shapes=[
                pltpu.VMEM((width, hid), bf16),
                pltpu.VMEM((width, hid), bf16),
                pltpu.VMEM((hid, width), bf16),
                pltpu.VMEM((n_line, tok, lanes), jnp.float32),
                pltpu.VMEM((CHUNKS, n_line, tok, cols), bf16),
                pltpu.VMEM((CHUNKS, n_expert, slots, cols), bf16),
                pltpu.VMEM((CHUNKS, CORES, n_expert, slots, cols), bf16),
                pltpu.VMEM((CORES * used, hid), jnp.float32),
                pltpu.VMEM((CORES * used, hid), jnp.float32),
                pltpu.VMEM((CORES * used, hid), bf16),
                pltpu.VMEM((CHUNKS, n_expert, slots, cols), bf16),
                pltpu.VMEM((CHUNKS, n_expert, slots, cols), bf16),
                pltpu.VMEM((CHUNKS, n_expert, slots, cols), bf16),
                pltpu.VMEM((CHUNKS, n_line, tok, cols), bf16),
                pltpu.VMEM((CHUNKS, n_line, tok, cols), bf16),
                dma((3, CHUNKS)),
                dma((n_line - 1,)), dma((n_line - 1,)),
                dma(line), dma(line),
                dma(plane), dma(plane),
                dma((CHUNKS, n_expert)), dma((CHUNKS, n_expert)),
                dma((CHUNKS,)), dma((CHUNKS,)),
                dma(plane), dma(plane),
                dma(line), dma(line),
            ],
            compiler_params=pltpu.CompilerParams(
                collective_id=0, has_side_effects=True, vmem_limit_bytes=67043328
            ),
        )(tokens, norm_gain[None], routes, gate_weights, capacity, w_gate, w_up, w_down)

    return jax.shard_map(
        on_device,
        mesh=mesh,
        in_specs=(
            P(("expert", "shard"), None), P(), P(("expert", "shard"), None), P(("expert", "shard"), None), P(),
            P("expert", None, "shard"), P("expert", None, "shard"), P("expert", "shard", None),
        ),
        out_specs=P(("expert", "shard"), None),
        check_vma=False,
    )
```

```python
import functools

import jax
import jax.numpy as jnp
from jax import lax
from jax.experimental import pallas as pl
from jax.experimental.pallas import tpu as pltpu
from jax.sharding import PartitionSpec as P

CHUNKS = 3
EPS = 1e-05
MESH = pl.DeviceIdType.MESH
CORES = 2


def column_tile(width, most):
    tile = most
    while width % tile:
        tile //= 2
    return tile


def kernel(
    n_expert, n_line, depth,
    tokens, gain, routes, gates, capacity, gate_hbm, up_hbm, down_hbm, out,
    gate_w, up_w, down_w, meta, normed, picked, rows, acc_gate, acc_up, hidden, partner, summed, returned, mixed, final,
    w_sem, meta_send, meta_recv, line_send, line_recv, plane_send, plane_recv, relay_send, relay_recv,
    pair_send, pair_recv, back_send, back_recv, home_send, home_recv,
):
    expert = lax.axis_index("expert")
    shard = lax.axis_index("shard")
    place, core = shard // CORES, lax.rem(shard, CORES)
    other = 1 - core
    tok, width = tokens.shape
    cols = width // CHUNKS
    slots = n_line * depth
    used = n_expert * slots
    lanes = meta.shape[2]
    hid = gate_w.shape[1]
    total_rows = CORES * used

    def line_at(step):
        return lax.rem(place + step + n_line, n_line)

    def expert_at(step):
        return lax.rem(expert + step + n_expert, n_expert)

    def line_device(step):
        return {"expert": expert, "shard": line_at(step) * CORES + core}

    def plane_device(step):
        return {"expert": expert_at(step), "shard": shard}

    partner_device = {"expert": expert, "shard": place * CORES + other}
    peers = [line_device(d) for d in range(1, n_line)] + [plane_device(d) for d in range(1, n_expert)] + [partner_device]

    barrier = pltpu.get_barrier_semaphore()
    for peer in peers:
        pl.semaphore_signal(barrier, inc=1, device_id=peer, device_id_type=MESH)

    def weight_copy(kind, step):
        span = pl.ds(step * cols, cols)
        if kind == 0:
            return pltpu.make_async_copy(gate_hbm.at[0, span, :], gate_w.at[span, :], w_sem.at[0, step])
        if kind == 1:
            return pltpu.make_async_copy(up_hbm.at[0, span, :], up_w.at[span, :], w_sem.at[1, step])
        return pltpu.make_async_copy(down_hbm.at[0, :, span], down_w.at[:, span], w_sem.at[2, step])

    for step in range(CHUNKS):
        weight_copy(0, step).start()
        weight_copy(1, step).start()
    for step in range(CHUNKS):
        weight_copy(2, step).start()

    lane = lax.broadcasted_iota(jnp.int32, (tok, lanes), 1)
    row = lax.broadcasted_iota(jnp.int32, (tok, lanes), 0)
    lane_expert = lane // slots
    lane_slot = lax.rem(lane, depth)
    diagonal = lax.broadcasted_iota(jnp.int32, (tok, tok), 0) == lax.broadcasted_iota(jnp.int32, (tok, tok), 1)

    def column(ref, k):
        return jnp.sum(jnp.where(diagonal, ref[k : k + 1, :].astype(jnp.float32), 0.0), axis=1, keepdims=True)

    expert_of_lane = lane_expert.astype(jnp.float32)
    named = jnp.zeros((tok, lanes), jnp.float32)
    weight = jnp.zeros((tok, lanes), jnp.float32)
    for k in range(routes.shape[0]):
        this = column(routes, k) == expert_of_lane
        named = jnp.where(this, 1.0, named)
        weight = jnp.where(this, column(gates, k), weight)
    rank = jnp.zeros((tok, lanes), jnp.float32)
    for t in range(tok - 1):
        rank = rank + jnp.where(row > t, named[t : t + 1, :], 0.0)
    limit = jnp.zeros((tok, lanes), jnp.int32)
    for e in range(n_expert):
        limit = jnp.where(lane_expert == e, capacity[e], limit)
    rank = rank.astype(jnp.int32)
    keep = (named > 0.0) & (rank == lane_slot) & (rank < limit)
    meta[place] = jnp.where(keep, weight, 0.0)

    wide = tokens[...].astype(jnp.float32)
    scale = lax.rsqrt(jnp.mean(wide * wide, axis=-1, keepdims=True) + EPS)
    values = (wide * scale * gain[...]).astype(jnp.bfloat16)
    for step in range(CHUNKS):
        normed[step, place] = values[:, step * cols : (step + 1) * cols]

    pl.semaphore_wait(barrier, len(peers))
    sent = []

    def remote(src, dst, send, recv, device):
        return pltpu.make_async_remote_copy(
            src_ref=src, dst_ref=dst, send_sem=send, recv_sem=recv, device_id=device, device_id_type=MESH
        )

    def send(*args):
        copy = remote(*args)
        copy.start()
        return copy

    for d in range(1, n_line):
        sent.append(send(meta.at[place], meta.at[place], meta_send.at[d - 1], meta_recv.at[d - 1], line_device(d)))
    for step in range(CHUNKS):
        for d in range(1, n_line):
            block = normed.at[step, place]
            sent.append(send(block, block, line_send.at[step, d - 1], line_recv.at[step, d - 1], line_device(d)))
    for d in range(1, n_line):
        block = meta.at[line_at(-d)]
        remote(block, block, meta_send.at[d - 1], meta_recv.at[d - 1], line_device(-d)).wait_recv()

    tall = n_line * tok
    all_meta = meta[...].reshape(tall, lanes)
    lane = lax.broadcasted_iota(jnp.int32, (tall, lanes), 1)
    row = lax.broadcasted_iota(jnp.int32, (tall, lanes), 0)
    combine = jnp.where(lax.rem(lane // depth, n_line) == row // tok, all_meta, 0.0)
    picker = (combine != 0.0).astype(jnp.float32).T[:used].astype(jnp.bfloat16)
    combine = combine.astype(jnp.bfloat16)[:, :used]

    tile = column_tile(cols, 512)
    relays = []

    def pick(step):
        for d in range(1, n_line):
            block = normed.at[step, line_at(-d)]
            remote(block, block, line_send.at[step, d - 1], line_recv.at[step, d - 1], line_device(-d)).wait_recv()

        def body(i, _):
            span = pl.ds(pl.multiple_of(i * tile, tile), tile)
            gathered = normed[step, :, :, span].astype(jnp.float32).reshape(tall, tile).astype(jnp.bfloat16)
            chosen = jnp.dot(picker, gathered, preferred_element_type=jnp.float32)
            picked[step, :, :, span] = chosen.astype(jnp.bfloat16).reshape(n_expert, slots, tile)
            return 0

        lax.fori_loop(0, cols // tile, body, 0)
        for d in range(1, n_expert):
            sent.append(
                send(
                    picked.at[step, expert_at(d)], rows.at[step, core, expert],
                    plane_send.at[step, d - 1], plane_recv.at[step, d - 1], plane_device(d),
                )
            )
        rows[step, core, expert] = picked[step, expert]
        block = rows.at[step, core, expert]
        relays.append(send(picked.at[step, expert], block, relay_send.at[step, 0], relay_recv.at[step, 0], partner_device))

    def relay(step):
        for d in range(1, n_expert):
            block = rows.at[step, core, expert_at(-d)]
            remote(block, block, plane_send.at[step, d - 1], plane_recv.at[step, d - 1], plane_device(-d)).wait_recv()
            relays.append(send(block, block, relay_send.at[step, d], relay_recv.at[step, d], partner_device))

    hid_tile = column_tile(hid, 256)

    def project(step):
        for d in range(n_expert):
            block = rows.at[step, other, expert_at(-d)]
            remote(block, block, relay_send.at[step, d], relay_recv.at[step, d], partner_device).wait_recv()
        weight_copy(0, step).wait()
        weight_copy(1, step).wait()

        def body(i, _):
            span = pl.ds(pl.multiple_of(i * hid_tile, hid_tile), hid_tile)
            x = rows[step].reshape(total_rows, cols)
            depth_span = pl.ds(step * cols, cols)
            g = jnp.dot(x, gate_w[depth_span, span], preferred_element_type=jnp.float32)
            u = jnp.dot(x, up_w[depth_span, span], preferred_element_type=jnp.float32)
            if step > 0:
                g = g + acc_gate[:, span]
                u = u + acc_up[:, span]
            if step < CHUNKS - 1:
                acc_gate[:, span] = g
                acc_up[:, span] = u
            else:
                hidden[:, span] = (g / (1.0 + jnp.exp(-g)) * u).astype(jnp.bfloat16)
            return 0

        lax.fori_loop(0, hid // hid_tile, body, 0)

    for i in range(CHUNKS + 2):
        if i < CHUNKS:
            pick(i)
        if 0 <= i - 1 < CHUNKS:
            relay(i - 1)
        if 0 <= i - 2 < CHUNKS:
            project(i - 2)
    for copy in relays:
        copy.wait_send()

    def down(step):
        weight_copy(2, step).wait()

        def body(i, _):
            span = pl.ds(pl.multiple_of(i * tile, tile), tile)
            w_span = pl.ds(pl.multiple_of(step * cols + i * tile, tile), tile)
            y = jnp.dot(hidden[...], down_w[:, w_span], preferred_element_type=jnp.float32)
            rows[step, :, :, :, span] = y.astype(jnp.bfloat16).reshape(CORES, n_expert, slots, tile)
            return 0

        lax.fori_loop(0, cols // tile, body, 0)
        sent.append(send(rows.at[step, other], partner.at[step], pair_send.at[step], pair_recv.at[step], partner_device))

    def pair(step):
        remote(rows.at[step, core], partner.at[step], pair_send.at[step], pair_recv.at[step], partner_device).wait_recv()
        for d in range(n_expert):
            e = expert_at(d)
            both = rows[step, core, e].astype(jnp.float32) + partner[step, e].astype(jnp.float32)
            if d == 0:
                returned[step, e] = both.astype(jnp.bfloat16)
            else:
                summed[step, e] = both.astype(jnp.bfloat16)
                sent.append(
                    send(
                        summed.at[step, e], returned.at[step, expert],
                        back_send.at[step, d - 1], back_recv.at[step, d - 1], plane_device(d),
                    )
                )

    def mix(step):
        for d in range(1, n_expert):
            block = returned.at[step, expert_at(-d)]
            remote(block, block, back_send.at[step, d - 1], back_recv.at[step, d - 1], plane_device(-d)).wait_recv()

        def body(i, _):
            span = pl.ds(pl.multiple_of(i * tile, tile), tile)
            r = returned[step, :, :, span].reshape(used, tile)
            o = jnp.dot(combine, r, preferred_element_type=jnp.float32)
            mixed[step, :, :, span] = o.reshape(n_line, tok, tile).astype(jnp.bfloat16)
            return 0

        lax.fori_loop(0, cols // tile, body, 0)
        for d in range(1, n_line):
            sent.append(
                send(
                    mixed.at[step, line_at(d)], final.at[step, place],
                    home_send.at[step, d - 1], home_recv.at[step, d - 1], line_device(d),
                )
            )

    def finish(step):
        total = mixed[step, place].astype(jnp.float32)
        for d in range(1, n_line):
            block = final.at[step, line_at(-d)]
            remote(block, block, home_send.at[step, d - 1], home_recv.at[step, d - 1], line_device(-d)).wait_recv()
        for d in range(1, n_line):
            total = total + final[step, line_at(-d)].astype(jnp.float32)
        out[:, step * cols : (step + 1) * cols] = total.astype(jnp.bfloat16)

    for i in range(CHUNKS + 1):
        if i < CHUNKS:
            down(i)
        if 0 <= i - 1 < CHUNKS:
            pair(i - 1)
    for i in range(CHUNKS):
        mix(i)
    for i in range(CHUNKS):
        finish(i)
    for copy in sent:
        copy.wait_send()


def solution(mesh):
    n_expert = mesh.shape["expert"]
    n_line = mesh.shape["shard"] // CORES

    def on_device(tokens, norm_gain, routes, gate_weights, capacity, w_gate, w_up, w_down):
        tok, width = tokens.shape
        hid = w_gate.shape[2]
        depth = max(tok // 2, tok * routes.shape[1] // n_expert)
        cols = width // CHUNKS
        slots = n_line * depth
        used = n_expert * slots
        lanes = -(-used // 128) * 128
        dma = pltpu.SemaphoreType.DMA
        bf16 = jnp.bfloat16
        vmem = pl.BlockSpec(memory_space=pltpu.VMEM)
        hbm = pl.BlockSpec(memory_space=pl.ANY)
        line, plane = (CHUNKS, n_line - 1), (CHUNKS, n_expert - 1)
        return pl.pallas_call(
            functools.partial(kernel, n_expert, n_line, depth),
            out_shape=jax.ShapeDtypeStruct((tok, width), bf16),
            in_specs=[vmem, vmem, vmem, vmem, pl.BlockSpec(memory_space=pltpu.SMEM), hbm, hbm, hbm],
            out_specs=vmem,
            scratch_shapes=[
                pltpu.VMEM((width, hid), bf16),
                pltpu.VMEM((width, hid), bf16),
                pltpu.VMEM((hid, width), bf16),
                pltpu.VMEM((n_line, tok, lanes), jnp.float32),
                pltpu.VMEM((CHUNKS, n_line, tok, cols), bf16),
                pltpu.VMEM((CHUNKS, n_expert, slots, cols), bf16),
                pltpu.VMEM((CHUNKS, CORES, n_expert, slots, cols), bf16),
                pltpu.VMEM((CORES * used, hid), jnp.float32),
                pltpu.VMEM((CORES * used, hid), jnp.float32),
                pltpu.VMEM((CORES * used, hid), bf16),
                pltpu.VMEM((CHUNKS, n_expert, slots, cols), bf16),
                pltpu.VMEM((CHUNKS, n_expert, slots, cols), bf16),
                pltpu.VMEM((CHUNKS, n_expert, slots, cols), bf16),
                pltpu.VMEM((CHUNKS, n_line, tok, cols), bf16),
                pltpu.VMEM((CHUNKS, n_line, tok, cols), bf16),
                dma((3, CHUNKS)),
                dma((n_line - 1,)), dma((n_line - 1,)),
                dma(line), dma(line),
                dma(plane), dma(plane),
                dma((CHUNKS, n_expert)), dma((CHUNKS, n_expert)),
                dma((CHUNKS,)), dma((CHUNKS,)),
                dma(plane), dma(plane),
                dma(line), dma(line),
            ],
            compiler_params=pltpu.CompilerParams(
                collective_id=0, has_side_effects=True, vmem_limit_bytes=67043328
            ),
        )(tokens, norm_gain[None], routes.T, gate_weights.T, capacity, w_gate, w_up, w_down)

    return jax.shard_map(
        on_device,
        mesh=mesh,
        in_specs=(
            P(("expert", "shard"), None), P(), P(("expert", "shard"), None), P(("expert", "shard"), None), P(),
            P("expert", None, "shard"), P("expert", None, "shard"), P("expert", "shard", None),
        ),
        out_specs=P(("expert", "shard"), None),
        check_vma=False,
    )
```
